8 devices in a mesh: rep: 2 (over y, z), dp: 4 (over x, core).
Axes of the slice: x: 2, y: 2, z: 1, core: 2. Of those that a mesh axis runs over, the one named last changes fastest.
Arguments:
- x: bfloat16 [8, 2048, 896], P(('rep', 'dp')), parts along dimension 0
- dy: bfloat16 [8, 2048, 896], P(('rep', 'dp')), parts along dimension 0
- w_gate: bfloat16 [2, 896, 2560], replicated
- w_up: bfloat16 [2, 896, 2560], replicated
- w_down: bfloat16 [2, 2560, 896], replicated
- m_w_gate: float32 [2, 896, 2560], replicated
- m_w_up: float32 [2, 896, 2560], replicated
- m_w_down: float32 [2, 2560, 896], replicated
- v_w_gate: float32 [2, 896, 2560], replicated
- v_w_up: float32 [2, 896, 2560], replicated
- v_w_down: float32 [2, 2560, 896], replicated
Outputs:
- output 1: bfloat16 [4, 896, 2560], P('rep'), parts along dimension 0
- output 2: bfloat16 [4, 896, 2560], P('rep'), parts along dimension 0
- output 3: bfloat16 [4, 2560, 896], P('rep'), parts along dimension 0
- output 4: float32 [4, 896, 2560], P('rep'), parts along dimension 0
- output 5: float32 [4, 896, 2560], P('rep'), parts along dimension 0
- output 6: float32 [4, 2560, 896], P('rep'), parts along dimension 0
- output 7: float32 [4, 896, 2560], P('rep'), parts along dimension 0
- output 8: float32 [4, 896, 2560], P('rep'), parts along dimension 0
- output 9: float32 [4, 2560, 896], P('rep'), parts along dimension 0
There are 2 independent parts. The reference program is written for one: setup_inputs(seed, part) draws one part's arguments, and reference() takes and returns one part's arrays. A program takes and returns all parts, laid end to end along the dimension named above; an argument that names none is the same for every part.
All inputs are finite; a program needn't handle non-finite values.
Results may differ from the reference program's by a relative error of at most 0.022.
Values are sent between devices in bfloat16 or wider.
A program may use at most 2.5 GiB of HBM per device.

```python
import jax
import jax.numpy as jnp
from jax import lax

SEQUENCES = 4
TOKENS = 2048
D = 896
FF = 2560
LAYERS = 2
NAMES = ("w_gate", "w_up", "w_down")
SHAPES = {"w_gate": (LAYERS, D, FF), "w_up": (LAYERS, D, FF), "w_down": (LAYERS, FF, D)}


def bump(key, n, height):
    away = (jnp.arange(n, dtype=jnp.int32) - jax.random.randint(key, (), 0, n, jnp.int32)) % n
    return jnp.where(away < n // 8, height, 1.0)


def together(key, own, strength):
    shared = jax.random.normal(key, own.shape[1:], jnp.float32)
    return (own + strength * shared) * lax.rsqrt(1 + strength * strength)


def setup_inputs(seed: int = 0, part: int = 0) -> dict:
    kx, kdy, ka, kb, kz, kf, kh, kl, *keys = jax.random.split(jax.random.key(seed), 8 + 3 * len(NAMES))
    kx, kdy, ka, kb = (jax.random.fold_in(k, part) for k in (kx, kdy, ka, kb))
    kw, km, kv = (keys[i::3] for i in range(3))
    shape = (SEQUENCES, TOKENS, D)
    much_x, much_dy = jax.random.uniform(kz, (2,), jnp.float32, 0.0, 1.0)
    loud = 2.0 ** jax.random.uniform(jax.random.fold_in(kz, 1), (), jnp.float32, -1.0, 2.0)
    layers = 2.0 ** jax.random.uniform(kl, (LAYERS, 1, 1), jnp.float32, -1.0, 1.0)
    x = together(ka, jax.random.normal(kx, shape, jnp.float32), much_x) * bump(kf, D, 4.0)
    dy = together(kb, jax.random.normal(kdy, shape, jnp.float32), much_dy)
    drawn = {"x": x.astype(jnp.bfloat16), "dy": (loud * dy * (SEQUENCES * TOKENS) ** -0.5).astype(jnp.bfloat16)}
    for key, name in zip(kw, NAMES, strict=True):
        w = jax.random.normal(key, SHAPES[name], jnp.float32) * SHAPES[name][1] ** -0.5
        drawn[name] = (w * {"w_gate": 1.0, "w_up": bump(kh, FF, 4.0), "w_down": layers}[name]).astype(jnp.bfloat16)
    for key, name in zip(km, NAMES, strict=True):
        drawn[f"m_{name}"] = 0.1 * jax.random.normal(key, SHAPES[name], jnp.float32)
    for key, name in zip(kv, NAMES, strict=True):
        drawn[f"v_{name}"] = jax.random.uniform(key, SHAPES[name], jnp.float32, 0.005, 0.015)
    return drawn


def matmul(a, w):
    return jnp.dot(a, w, preferred_element_type=jnp.float32).astype(jnp.bfloat16)


def normed(h):
    wide = h.astype(jnp.float32)
    scale = lax.rsqrt(jnp.mean(wide**2, -1, keepdims=True) + 1e-6)
    return (wide * scale).astype(jnp.bfloat16)


def layer(h, w):
    a = normed(h)
    gate = jnp.dot(a, w["w_gate"], preferred_element_type=jnp.float32)
    up = jnp.dot(a, w["w_up"], preferred_element_type=jnp.float32)
    return h + matmul((jax.nn.silu(gate) * up).astype(jnp.bfloat16), w["w_down"])


def adamw(w, m, v, g):
    m = 0.9 * m + 0.1 * g
    v = 0.95 * v + 0.05 * g * g
    step = m * lax.rsqrt(v + 1e-8) + 0.1 * w
    return (w - 0.02 * step).astype(jnp.bfloat16), m, v


def clipped(gradients, sum_of_squares, count):
    factor = jnp.minimum(1.0, 0.5 * lax.rsqrt(sum_of_squares / count + 1e-30))
    return [g * factor for g in gradients]


def stack(weights, h):
    return lax.scan(lambda h, w: (layer(h, w), None), h, weights)[0]


def reference(x, dy, w_gate, w_up, w_down, m_w_gate, m_w_up, m_w_down, v_w_gate, v_w_up, v_w_down):
    weights = dict(zip(NAMES, (w_gate, w_up, w_down), strict=True))

    def take(so_far, sequence):
        h, by_y = sequence
        _, back = jax.vjp(lambda w: stack(w, h), weights)
        return jax.tree.map(lambda total, term: total + term.astype(jnp.float32), so_far, back(by_y)[0]), None

    none_yet = {name: jnp.zeros(w.shape, jnp.float32) for name, w in weights.items()}
    by_weights, _ = lax.scan(take, none_yet, (x, dy))
    gradients = [by_weights[name].astype(jnp.bfloat16).astype(jnp.float32) for name in NAMES]
    gradients = clipped(gradients, sum(jnp.sum(g * g) for g in gradients), sum(g.size for g in gradients))
    new = [
        adamw(w.astype(jnp.float32), m, v, g)
        for w, m, v, g in zip((w_gate, w_up, w_down), (m_w_gate, m_w_up, m_w_down), (v_w_gate, v_w_up, v_w_down), gradients, strict=True)
    ]
    return tuple(one[which] for which in range(3) for one in new)
```

```python
import functools

import jax
import jax.numpy as jnp
from jax import lax
from jax.experimental import pallas as pl
from jax.experimental.pallas import tpu as pltpu
from jax.sharding import PartitionSpec as P

MESH = pl.DeviceIdType.MESH
F32, BF16 = jnp.float32, jnp.bfloat16
TOKENS, D, FF, LAYERS = 2048, 896, 2560, 2
T = 256
NT = FF // T
TILES = LAYERS * NT
ROWS = 512
HALF, QUARTER = D // 2, D // 4
LAG = 5
COUNT = 3 * LAYERS * D * FF


def dot(a, b, ca, cb):
    return lax.dot_general(a, b, (((ca,), (cb,)), ((), ())), preferred_element_type=F32)


def normed(h):
    wide = h.astype(F32)
    return (wide * lax.rsqrt(jnp.mean(wide * wide, -1, keepdims=True) + 1e-6)).astype(BF16)


def lanes(sq):
    by_row = jnp.sum(sq.reshape(sq.shape[0] // 8, 8, sq.shape[1]), axis=0)
    return sum(by_row[:, i * 128 : (i + 1) * 128] for i in range(sq.shape[1] // 128))


def grads_kernel(
    x_hbm, dy_hbm, wg, wu, wd,
    gate1, up1, down1, gate0, up0, down0, factor,
    x, h, dy, a, acc, hs, dgs, dus,
    mine_gu, mine_d, r1_gu, r1_d, xs_gu, xs_d, xk_gu, xk_d, r2_gu, r2_d, squares, ss_all,
    in_sem, d_send, d_recv, x_send, x_recv, out_sem, s_send, s_recv,
):
    s = pl.program_id(0)
    me, rep = lax.axis_index("dp"), lax.axis_index("rep")
    core, chip = lax.rem(me, 2), lax.div(me, 2)
    partner, across = me + 1 - 2 * core, lax.rem(me + 2, 4)
    t = s - NT

    def rows_loop(body):
        for i in range(TOKENS // ROWS):
            body(pl.ds(i * ROWS, ROWS))

    def to_partner(t):
        slot = lax.rem(t, 2)
        theirs = pl.ds(pl.multiple_of((1 - core) * HALF, 64), HALF)
        theirs_d = pl.ds(pl.multiple_of((1 - core) * (T // 2), 64), T // 2)
        make = functools.partial(pltpu.make_async_remote_copy, device_id=(rep, partner), device_id_type=MESH)
        return (
            make(mine_gu.at[slot, :, theirs, :], r1_gu.at[slot], d_send.at[slot, 0], d_recv.at[slot, 0]),
            make(mine_d.at[slot, theirs_d, :], r1_d.at[slot], d_send.at[slot, 1], d_recv.at[slot, 1]),
        )

    def to_across(t):
        slot = lax.rem(t, LAG + 1)
        make = functools.partial(pltpu.make_async_remote_copy, device_id=(rep, across), device_id_type=MESH)
        return (
            make(xs_gu.at[slot], r2_gu.at[t], x_send.at[slot, 0], x_recv.at[t, 0]),
            make(xs_d.at[slot], r2_d.at[t], x_send.at[slot, 1], x_recv.at[t, 1]),
        )

    def outs(t, refs):
        j = lax.rem(t, NT)
        cols = pl.ds(pl.multiple_of(j * T, T), T)
        rows = pl.ds(pl.multiple_of(j * (T // 4), T // 4), T // 4)
        return (
            pltpu.make_async_copy(r2_gu.at[t, 0], refs[0].at[:, cols], out_sem.at[t, 0]),
            pltpu.make_async_copy(r2_gu.at[t, 1], refs[1].at[:, cols], out_sem.at[t, 1]),
            pltpu.make_async_copy(r2_d.at[t], refs[2].at[rows, :], out_sem.at[t, 2]),
        )

    def chip_sum(t):
        slot, xslot = lax.rem(t, 2), lax.rem(t, LAG + 1)
        for c in to_partner(t):
            c.wait()
        for keep in (True, False):
            q = chip if keep else 1 - chip
            mine = pl.ds(pl.multiple_of(core * HALF + q * QUARTER, 32), QUARTER)
            got = pl.ds(pl.multiple_of(q * QUARTER, 32), QUARTER)
            mine_rows = pl.ds(pl.multiple_of(core * (T // 2) + q * (T // 4), 64), T // 4)
            got_rows = pl.ds(pl.multiple_of(q * (T // 4), 64), T // 4)
            to_gu, to_d = (xk_gu, xk_d) if keep else (xs_gu, xs_d)
            for i in range(2):
                total = mine_gu[slot, i, mine, :].astype(F32) + r1_gu[slot, i, got, :].astype(F32)
                to_gu[xslot, i] = total.astype(to_gu.dtype)
            total = mine_d[slot, mine_rows, :].astype(F32) + r1_d[slot, got_rows, :].astype(F32)
            to_d[xslot] = total.astype(to_d.dtype)
        for c in to_across(t):
            c.start()

    def finish(t):
        xslot = lax.rem(t, LAG + 1)
        for c in to_across(t):
            c.wait()
        part = squares[...]
        for i in range(2):
            g = (xk_gu[xslot, i] + r2_gu[t, i].astype(F32)).astype(BF16)
            r2_gu[t, i] = g
            g = g.astype(F32)
            part += lanes(g * g)
        g = (xk_d[xslot] + r2_d[t].astype(F32)).astype(BF16)
        r2_d[t] = g
        g = g.astype(F32)
        squares[...] = part + lanes(g * g)

        @pl.when(t < NT)
        def _():
            for c in outs(t, (gate1, up1, down1)):
                c.start()

        @pl.when(t >= NT)
        def _():
            for c in outs(t, (gate0, up0, down0)):
                c.start()

    @pl.when(s == 0)
    def _():
        barrier = pltpu.get_barrier_semaphore()
        for k in range(1, 4):
            pl.semaphore_signal(barrier, inc=1, device_id=(rep, lax.rem(me + k, 4)), device_id_type=MESH)
        load_x = pltpu.make_async_copy(x_hbm, x, in_sem.at[0])
        load_dy = pltpu.make_async_copy(dy_hbm, dy, in_sem.at[1])
        load_x.start()
        load_dy.start()
        load_x.wait()
        squares[...] = jnp.zeros_like(squares)

        def start(r):
            a[r, :] = normed(x[r, :])
            acc[r, :] = jnp.zeros((ROWS, D), F32)

        rows_loop(start)
        load_dy.wait()
        pl.semaphore_wait(barrier, 3)

    @pl.when(s < NT)
    def _():
        def forward(r):
            gate = dot(a[r, :], wg[...], 1, 0)
            up = dot(a[r, :], wu[...], 1, 0)
            hidden = (gate * jax.nn.sigmoid(gate) * up).astype(BF16)
            acc[r, :] += dot(hidden, wd[...], 1, 0)

        rows_loop(forward)

    @pl.when(s == NT)
    def _():
        def between(r):
            h[r, :] = x[r, :] + acc[r, :].astype(BF16)
            a[r, :] = normed(h[r, :])
            acc[r, :] = jnp.zeros((ROWS, D), F32)

        rows_loop(between)

    @pl.when(s == 2 * NT)
    def _():
        def between(r):
            da = acc[r, :].astype(BF16).astype(F32)
            wide = h[r, :].astype(F32)
            scale = lax.rsqrt(jnp.mean(wide * wide, -1, keepdims=True) + 1e-6)
            along = jnp.mean(da * wide, -1, keepdims=True)
            by_norm = da * scale - wide * (scale * scale * scale * along)
            dy[r, :] = dy[r, :] + by_norm.astype(BF16)
            a[r, :] = normed(x[r, :])

        rows_loop(between)

    @pl.when(s >= NT)
    def _():
        def hidden_grads(r):
            gate = dot(a[r, :], wg[...], 1, 0)
            up = dot(a[r, :], wu[...], 1, 0)
            dhid = dot(dy[r, :], wd[...], 1, 1).astype(BF16).astype(F32)
            sig = jax.nn.sigmoid(gate)
            silu = gate * sig
            hs[r, :] = (silu * up).astype(BF16)
            dus[r, :] = (dhid * silu).astype(BF16)
            dgs[r, :] = (dhid * up * (sig + silu * (1 - sig))).astype(BF16)

        rows_loop(hidden_grads)

        @pl.when(s < 2 * NT)
        def _():
            def input_grads(r):
                by_both = jnp.concatenate([dgs[r, :], dus[r, :]], 1)
                acc[r, :] += dot(by_both, jnp.concatenate([wg[...], wu[...]], 1), 1, 1)

            rows_loop(input_grads)

        @pl.when(t >= 1)
        def _():
            chip_sum(t - 1)

        slot = lax.rem(t, 2)
        mine_d[slot] = dot(hs[...], dy[...], 0, 0).astype(BF16)
        mine_gu[slot, 0] = dot(a[...], dgs[...], 0, 0).astype(BF16)
        mine_gu[slot, 1] = dot(a[...], dus[...], 0, 0).astype(BF16)
        for c in to_partner(t):
            c.start()

        @pl.when(t >= LAG)
        def _():
            finish(t - LAG)

    @pl.when(s == NT + TILES - 1)
    def _():
        chip_sum(TILES - 1)
        lax.fori_loop(TILES - LAG, TILES, lambda i, c: (finish(i), c)[1], 0)
        ss_all[me] = squares[...]
        copies = [
            pltpu.make_async_remote_copy(
                squares, ss_all.at[me], s_send.at[k - 1], s_recv.at[me],
                device_id=(rep, lax.rem(me + k, 4)), device_id_type=MESH,
            )
            for k in range(1, 4)
        ]
        for c in copies:
            c.start()
        for c in copies:
            c.wait_send()
        for k in range(1, 4):
            who = lax.rem(me + k, 4)
            pltpu.make_async_remote_copy(
                squares, ss_all.at[who], s_send.at[k - 1], s_recv.at[who], device_id=(rep, who), device_id_type=MESH
            ).wait_recv()
        total = jnp.sum((ss_all[0] + ss_all[1]) + (ss_all[2] + ss_all[3]))
        factor[...] = jnp.minimum(1.0, 0.5 * lax.rsqrt(jnp.full((8, 128), total / COUNT + 1e-30, F32)))
        lax.fori_loop(0, NT, lambda i, c: ([o.wait() for o in outs(i, (gate1, up1, down1))], c)[1], 0)
        lax.fori_loop(NT, TILES, lambda i, c: ([o.wait() for o in outs(i, (gate0, up0, down0))], c)[1], 0)


def gradients(x, dy, w_gate, w_up, w_down):
    any_space = pl.BlockSpec(memory_space=pl.ANY)
    layer = lambda s: lax.rem(lax.div(s, NT), 2)
    across = pl.BlockSpec((None, D, T), lambda s: (layer(s), 0, lax.rem(s, NT)))
    down = pl.BlockSpec((None, T, D), lambda s: (layer(s), lax.rem(s, NT), 0))
    wide, tall = jax.ShapeDtypeStruct((QUARTER, FF), BF16), jax.ShapeDtypeStruct((FF // 4, D), BF16)
    V, DMA = pltpu.VMEM, pltpu.SemaphoreType.DMA
    return pl.pallas_call(
        grads_kernel,
        grid=(NT + TILES,),
        out_shape=(wide, wide, tall, wide, wide, tall, jax.ShapeDtypeStruct((8, 128), F32)),
        in_specs=[any_space, any_space, across, across, down],
        out_specs=[any_space] * 6 + [pl.BlockSpec((8, 128), lambda s: (0, 0))],
        scratch_shapes=[
            V((TOKENS, D), BF16), V((TOKENS, D), BF16), V((TOKENS, D), BF16), V((TOKENS, D), BF16), V((TOKENS, D), F32),
            V((TOKENS, T), BF16), V((TOKENS, T), BF16), V((TOKENS, T), BF16),
            V((2, 2, D, T), BF16), V((2, T, D), BF16),
            V((2, 2, HALF, T), BF16), V((2, T // 2, D), BF16),
            V((LAG + 1, 2, QUARTER, T), BF16), V((LAG + 1, T // 4, D), BF16),
            V((LAG + 1, 2, QUARTER, T), F32), V((LAG + 1, T // 4, D), F32),
            V((TILES, 2, QUARTER, T), BF16), V((TILES, T // 4, D), BF16),
            V((8, 128), F32), V((4, 8, 128), F32),
            DMA((2,)), DMA((2, 2)), DMA((2, 2)), DMA((LAG + 1, 2)), DMA((TILES, 2)), DMA((TILES, 3)), DMA((3,)), DMA((4,)),
        ],
        compiler_params=pltpu.CompilerParams(
            collective_id=0, has_side_effects=True, vmem_limit_bytes=67_000_000, dimension_semantics=("arbitrary",)
        ),
        cost_estimate=pl.CostEstimate(flops=17 * 2 * TOKENS * D * FF, bytes_accessed=100_000_000, transcendentals=0),
        name="grads",
    )(x, dy, w_gate, w_up, w_down)


def adamw_kernel(rows, pos, factor, q0, q1, q2, q3, w, m, v, *refs):
    new_w, new_m, new_v = refs[-3:]
    scale = factor[0, 0]
    for k, q in enumerate((q0, q1, q2, q3)):
        at = pl.ds(pl.multiple_of(pos[k] * rows, 32), rows)
        g = q[...].astype(F32) * scale
        m1 = 0.9 * m[at, :] + 0.1 * g
        v1 = 0.95 * v[at, :] + 0.05 * g * g
        w0 = w[at, :].astype(F32)
        new_m[at, :] = m1
        new_v[at, :] = v1
        new_w[at, :] = (w0 - 0.02 * (m1 * lax.rsqrt(v1 + 1e-8) + 0.1 * w0)).astype(BF16)


def adamw(layer, pos, factor, quarters, w, m, v, so_far):
    if w.shape[1] == D:
        block, quarter = pl.BlockSpec((None, D, T), lambda j: (layer, 0, j)), pl.BlockSpec((QUARTER, T), lambda j: (0, j))
        rows = QUARTER
    else:
        block, quarter = pl.BlockSpec((None, T, D), lambda j: (layer, j, 0)), pl.BlockSpec((T // 4, D), lambda j: (j, 0))
        rows = T // 4
    smem = pl.BlockSpec(memory_space=pltpu.SMEM)
    return pl.pallas_call(
        functools.partial(adamw_kernel, rows),
        grid=(NT,),
        out_shape=tuple(jax.ShapeDtypeStruct(w.shape, d) for d in (BF16, F32, F32)),
        in_specs=[smem, smem] + [quarter] * 4 + [block] * 3 + [pl.BlockSpec(memory_space=pl.ANY)] * len(so_far),
        out_specs=[block] * 3,
        input_output_aliases={9 + i: i for i in range(len(so_far))},
        compiler_params=pltpu.CompilerParams(vmem_limit_bytes=32 * 2**20),
        cost_estimate=pl.CostEstimate(flops=15_000_000_000, bytes_accessed=22 * D * FF, transcendentals=0),
        name=f"adamw{layer}",
    )(pos, factor, *quarters, w, m, v, *so_far)


def solution(mesh):
    swap_cores = [(0, 1), (1, 0), (2, 3), (3, 2)]
    swap_chips = [(0, 2), (2, 0), (1, 3), (3, 1)]

    def step(x, dy, *arrays):
        weights, m, v = (arrays[i : i + 3] for i in (0, 3, 6))
        *mine, factor = gradients(x[0], dy[0], *weights)
        me = lax.axis_index("dp")
        core, chip = me % 2, me // 2
        pos = jnp.stack([core * 2 + chip, core * 2 + 1 - chip, (1 - core) * 2 + chip, (1 - core) * 2 + 1 - chip]).astype(jnp.int32)
        new, last = [(), (), ()], None
        for n, q in enumerate(mine):
            layer, which = 1 - n // 3, n % 3
            other = lax.ppermute(q, "dp", swap_chips)
            if last is not None:
                other, new[last] = lax.optimization_barrier((other, new[last]))
            quarters = (q, other, lax.ppermute(q, "dp", swap_cores), lax.ppermute(other, "dp", swap_cores))
            new[which] = adamw(layer, pos, factor[:1, :1], quarters, weights[which], m[which], v[which], new[which])
            last = which
        return tuple(one[i] for i in range(3) for one in new)

    return jax.shard_map(
        step,
        mesh=mesh,
        in_specs=(P(("rep", "dp"), None, None),) * 2 + (P(None, None, None),) * 9,
        out_specs=(P("rep", None, None),) * 9,
        check_vma=False,
    )
```

```python
import functools

import jax
import jax.numpy as jnp
from jax import lax
from jax.experimental import pallas as pl
from jax.experimental.pallas import tpu as pltpu
from jax.sharding import PartitionSpec as P


MESH = pl.DeviceIdType.MESH
F32, BF16 = jnp.float32, jnp.bfloat16
TOKENS, D, FF, LAYERS = 2048, 896, 2560, 2
T = 256
NT = FF // T
TILES = LAYERS * NT
ROWS = 512
HALF, QUARTER = D // 2, D // 4
LAG = 5
PIECES = ((0, 4), (4, 10), (10, 14), (14, 18), (18, 20))
N = len(PIECES)
EARLY = PIECES[0][1]
COUNT = 3 * LAYERS * D * FF
FOLD = [((slice(0, 64), slice(256 * i, 256 * i + 256)), (slice(64 * i, 64 * i + 64), slice(0, 256))) for i in range(3)] + [
    ((slice(32 * i, 32 * i + 32), slice(768, 896)), (slice(192, 224), slice(128 * i, 128 * i + 128))) for i in range(2)
]


def dot(a, b, ca, cb):
    return lax.dot_general(a, b, (((ca,), (cb,)), ((), ())), preferred_element_type=F32)


def normed(h):
    wide = h.astype(F32)
    return (wide * lax.rsqrt(jnp.mean(wide * wide, -1, keepdims=True) + 1e-6)).astype(BF16)


def lanes(sq):
    by_row = jnp.sum(sq.reshape(sq.shape[0] // 8, 8, sq.shape[1]), axis=0)
    return sum(by_row[:, i * 128 : (i + 1) * 128] for i in range(sq.shape[1] // 128))


def grads_kernel(
    x_hbm, dy_hbm, wg, wu, wd,
    *refs,
):
    own, sibling, other = refs[:3]
    pieces = refs[2 : 2 + N]
    (
    factor,
    x, h, dy, a, acc, hs, dgs, dus,
    mine_gu, mine_d, r1_gu, r1_d, xs, xk, r2, squares, ss_all,
    in_sem, d_send, d_recv, x_send, x_recv, out_sem, g_send, g_recv, e_send, e_recv, s_send, s_recv,
    ) = refs[2 + N :]
    s = pl.program_id(0)
    me, rep = lax.axis_index("dp"), lax.axis_index("rep")
    core, chip = lax.rem(me, 2), lax.div(me, 2)
    partner, across = me + 1 - 2 * core, lax.rem(me + 2, 4)
    t = s - NT

    def rows_loop(body, first=0, last=TOKENS):
        for i in range(first, last, ROWS):
            body(pl.ds(i, ROWS))

    def to_partner(t):
        slot = lax.rem(t, 2)
        theirs = pl.ds(pl.multiple_of((1 - core) * HALF, 64), HALF)
        theirs_d = pl.ds(pl.multiple_of((1 - core) * (T // 2), 64), T // 2)
        make = functools.partial(pltpu.make_async_remote_copy, device_id=(rep, partner), device_id_type=MESH)
        return (
            make(mine_gu.at[slot, :, theirs, :], r1_gu.at[slot], d_send.at[slot, 0], d_recv.at[slot, 0]),
            make(mine_d.at[slot, theirs_d, :], r1_d.at[slot], d_send.at[slot, 1], d_recv.at[slot, 1]),
        )

    def to_across(t):
        slot = lax.rem(t, LAG + 1)
        make = functools.partial(pltpu.make_async_remote_copy, device_id=(rep, across), device_id_type=MESH)
        return (make(xs.at[slot], r2.at[t + LAG], x_send.at[slot], x_recv.at[t]),)

    def outs(t, piece):
        first, src = PIECES[piece][0], r2.at[t + LAG]
        everywhere = pl.ds(pl.multiple_of(t * T, T), T)
        here = pl.ds(pl.multiple_of((t - first) * T, T), T)
        make = functools.partial(pltpu.make_async_remote_copy, device_id_type=MESH)
        copies = [
            pltpu.make_async_copy(src, own.at[:, :, everywhere], out_sem.at[t, 0]),
            make(src, sibling.at[:, :, everywhere], g_send.at[t], g_recv.at[t], device_id=(rep, partner)),
        ]
        if piece:
            copies.append(pltpu.make_async_copy(src, pieces[piece].at[:, :, here], out_sem.at[t, 1]))
        else:
            copies.append(make(src, other.at[:, :, here], e_send.at[t], e_recv.at[t], device_id=(rep, across)))
        return copies

    def chip_sum(t):
        slot, xslot = lax.rem(t + 2, 2), lax.rem(t + LAG + 1, LAG + 1)
        for keep in (True, False):
            q = chip if keep else 1 - chip
            mine = pl.ds(pl.multiple_of(core * HALF + q * QUARTER, 32), QUARTER)
            got = pl.ds(pl.multiple_of(q * QUARTER, 32), QUARTER)
            mine_rows = pl.ds(pl.multiple_of(core * (T // 2) + q * (T // 4), 64), T // 4)
            got_rows = pl.ds(pl.multiple_of(q * (T // 4), 64), T // 4)
            to = xk if keep else xs
            for i in range(2):
                total = mine_gu[slot, i, mine, :].astype(F32) + r1_gu[slot, i, got, :].astype(F32)
                to[xslot, i] = total.astype(to.dtype)
            total = (mine_d[slot, mine_rows, :].astype(F32) + r1_d[slot, got_rows, :].astype(F32)).astype(to.dtype)
            for (rows, cols), (at_rows, at_cols) in FOLD:
                to[xslot, 2, at_rows, at_cols] = total[rows, cols]

    def finish(t):
        xslot = lax.rem(t + LAG + 1, LAG + 1)
        part = squares[...]
        for i in range(3):
            g = (xk[xslot, i] + r2[t + LAG, i].astype(F32)).astype(BF16)
            r2[t + LAG, i] = g
            g = g.astype(F32)
            part += lanes(g * g)
        squares[...] = jnp.where(t >= 0, part, squares[...])

    def put_out(t):
        for piece, (first, last) in enumerate(PIECES):

            @pl.when((t >= first) & (t < last))
            def _():
                for c in outs(t, piece):
                    c.start()

    @pl.when(s == 0)
    def _():
        barrier = pltpu.get_barrier_semaphore()
        for k in range(1, 4):
            pl.semaphore_signal(barrier, inc=1, device_id=(rep, lax.rem(me + k, 4)), device_id_type=MESH)
        load_x = pltpu.make_async_copy(x_hbm, x, in_sem.at[0])
        load_dy = pltpu.make_async_copy(dy_hbm, dy, in_sem.at[1])
        load_x.start()
        load_dy.start()
        load_x.wait()
        squares[...] = jnp.zeros_like(squares)

        def start(r):
            a[r, :] = normed(x[r, :])
            acc[r, :] = jnp.zeros((ROWS, D), F32)

        rows_loop(start)
        load_dy.wait()
        pl.semaphore_wait(barrier, 3)

    @pl.when(s < NT)
    def _():
        def forward(r):
            gate = dot(a[r, :], wg[...], 1, 0)
            up = dot(a[r, :], wu[...], 1, 0)
            hidden = (gate * jax.nn.sigmoid(gate) * up).astype(BF16)
            acc[r, :] += dot(hidden, wd[...], 1, 0)

        rows_loop(forward)

    @pl.when(s == NT)
    def _():
        def between(r):
            h[r, :] = x[r, :] + acc[r, :].astype(BF16)
            a[r, :] = normed(h[r, :])
            acc[r, :] = jnp.zeros((ROWS, D), F32)

        rows_loop(between)

    @pl.when(s == 2 * NT)
    def _():
        def between(r):
            da = acc[r, :].astype(BF16).astype(F32)
            wide = h[r, :].astype(F32)
            scale = lax.rsqrt(jnp.mean(wide * wide, -1, keepdims=True) + 1e-6)
            along = jnp.mean(da * wide, -1, keepdims=True)
            by_norm = da * scale - wide * (scale * scale * scale * along)
            dy[r, :] = dy[r, :] + by_norm.astype(BF16)
            a[r, :] = normed(x[r, :])

        rows_loop(between)

    @pl.when(s >= NT)
    def _():
        def hidden_grads(r):
            gate = dot(a[r, :], wg[...], 1, 0)
            up = dot(a[r, :], wu[...], 1, 0)
            dhid = dot(dy[r, :], wd[...], 1, 1).astype(BF16).astype(F32)
            sig = jax.nn.sigmoid(gate)
            silu = gate * sig
            hs[r, :] = (silu * up).astype(BF16)
            dus[r, :] = (dhid * silu).astype(BF16)
            dgs[r, :] = (dhid * up * (sig + silu * (1 - sig))).astype(BF16)

        half = TOKENS // 2
        rows_loop(hidden_grads, 0, half)

        @pl.when(t >= 1)
        def _():
            for c in to_partner(t - 1):
                c.wait()

        rows_loop(hidden_grads, half, TOKENS)
        chip_sum(t - 1)

        @pl.when(t >= 1)
        def _():
            for c in to_across(t - 1):
                c.start()

        @pl.when(t >= LAG)
        def _():
            for c in to_across(t - LAG):
                c.wait()

        @pl.when(s < 2 * NT)
        def _():
            def input_grads(r):
                by_both = jnp.concatenate([dgs[r, :], dus[r, :]], 1)
                acc[r, :] += dot(by_both, jnp.concatenate([wg[...], wu[...]], 1), 1, 1)

            rows_loop(input_grads)

        slot = lax.rem(t, 2)
        finish(t - LAG)
        mine_d[slot] = dot(hs[...], dy[...], 0, 0).astype(BF16)
        mine_gu[slot, 0] = dot(a[...], dgs[...], 0, 0).astype(BF16)
        mine_gu[slot, 1] = dot(a[...], dus[...], 0, 0).astype(BF16)
        for c in to_partner(t):
            c.start()

        @pl.when(t >= LAG)
        def _():
            put_out(t - LAG)

    @pl.when(s == NT + TILES - 1)
    def _():
        for c in to_partner(TILES - 1):
            c.wait()
        chip_sum(TILES - 1)
        for c in to_across(TILES - 1):
            c.start()

        def rest(i, carry):
            for c in to_across(i):
                c.wait()
            finish(i)
            put_out(i)
            return carry

        lax.fori_loop(TILES - LAG, TILES, rest, 0)
        ss_all[me] = squares[...]
        copies = [
            pltpu.make_async_remote_copy(
                squares, ss_all.at[me], s_send.at[k - 1], s_recv.at[me],
                device_id=(rep, lax.rem(me + k, 4)), device_id_type=MESH,
            )
            for k in range(1, 4)
        ]
        for c in copies:
            c.start()
        for c in copies:
            c.wait_send()
        for k in range(1, 4):
            who = lax.rem(me + k, 4)
            pltpu.make_async_remote_copy(
                squares, ss_all.at[who], s_send.at[k - 1], s_recv.at[who], device_id=(rep, who), device_id_type=MESH
            ).wait_recv()
        total = jnp.sum((ss_all[0] + ss_all[1]) + (ss_all[2] + ss_all[3]))
        factor[...] = jnp.minimum(1.0, 0.5 * lax.rsqrt(jnp.full((8, 128), total / COUNT + 1e-30, F32)))
        for piece, (first, last) in enumerate(PIECES):
            lax.fori_loop(first, last, lambda i, c: ([o.wait() for o in outs(i, piece)], c)[1], 0)


def gradients(x, dy, w_gate, w_up, w_down):
    any_space = pl.BlockSpec(memory_space=pl.ANY)
    layer = lambda s: lax.rem(lax.div(s, NT), 2)
    across = pl.BlockSpec((None, D, T), lambda s: (layer(s), 0, lax.rem(s, NT)))
    down = pl.BlockSpec((None, T, D), lambda s: (layer(s), lax.rem(s, NT), 0))
    sizes = [TILES, TILES] + [last - first for first, last in PIECES]
    shapes = [jax.ShapeDtypeStruct((3, QUARTER, size * T), BF16) for size in sizes]
    V, DMA = pltpu.VMEM, pltpu.SemaphoreType.DMA
    *results, factor = pl.pallas_call(
        grads_kernel,
        grid=(NT + TILES,),
        out_shape=(*shapes, jax.ShapeDtypeStruct((8, 128), F32)),
        in_specs=[any_space, any_space, across, across, down],
        out_specs=[any_space] * len(shapes) + [pl.BlockSpec((8, 128), lambda s: (0, 0))],
        scratch_shapes=[
            V((TOKENS, D), BF16), V((TOKENS, D), BF16), V((TOKENS, D), BF16), V((TOKENS, D), BF16), V((TOKENS, D), F32),
            V((TOKENS, T), BF16), V((TOKENS, T), BF16), V((TOKENS, T), BF16),
            V((2, 2, D, T), BF16), V((2, T, D), BF16),
            V((2, 2, HALF, T), BF16), V((2, T // 2, D), BF16),
            V((LAG + 1, 3, QUARTER, T), BF16), V((LAG + 1, 3, QUARTER, T), F32), V((TILES + LAG, 3, QUARTER, T), BF16),
            V((8, 128), F32), V((4, 8, 128), F32),
            DMA((2,)), DMA((2, 2)), DMA((2, 2)), DMA((LAG + 1,)), DMA((TILES,)), DMA((TILES, 2)),
            DMA((TILES,)), DMA((TILES,)), DMA((EARLY,)), DMA((EARLY,)), DMA((3,)), DMA((4,)),
        ],
        compiler_params=pltpu.CompilerParams(
            collective_id=0, has_side_effects=True, vmem_limit_bytes=67_000_000, dimension_semantics=("arbitrary",)
        ),
        cost_estimate=pl.CostEstimate(flops=17 * 2 * TOKENS * D * FF, bytes_accessed=100_000_000, transcendentals=0),
        name="grads",
    )(x, dy, w_gate, w_up, w_down)
    own, sibling, early, *pieces = results
    return own, sibling, early, pieces, factor


def adamw_kernel(tiles, steps, pos, factor, *refs):
    *qs, refs = (*refs[: len(steps)], refs[len(steps) :])
    scale, j = factor[0, 0], pl.program_id(0)

    def update(which, at_q, *at):
        (w, m, v), (new_w, new_m, new_v) = refs[which:9:3], refs[-9:][which::3]
        g = qs[0][at_q] if len(qs) == 1 else jnp.where(j < steps[0], qs[0][at_q], qs[1][at_q])
        g = g.astype(F32) * scale
        m1 = 0.9 * m[at] + 0.1 * g
        v1 = 0.95 * v[at] + 0.05 * g * g
        w0 = w[at].astype(F32)
        new_m[at] = m1
        new_v[at] = v1
        new_w[at] = (w0 - 0.02 * (m1 * lax.rsqrt(v1 + 1e-8) + 0.1 * w0)).astype(BF16)

    for which in range(2):
        update(which, which, slice(None), slice(None))
    for i in range(tiles):
        for there, (rows, cols) in FOLD:
            update(2, (2, rows, slice(cols.start + i * T, cols.stop + i * T)), i, *there)


def adamw(tiles, parts, pos, factor, weights, m, v, so_far):
    steps = [(last - first) // tiles for first, last, _, _ in parts]

    def at(j):
        (first, _, whose, _), (first1, _, whose1, _) = parts[0], parts[-1]
        later = j >= steps[0]
        first = jnp.where(later, first1 - tiles * steps[0], first) + tiles * j
        return 1 - first // NT, first % NT // tiles, jnp.where(later, whose1, whose)

    def across_at(j, pos):
        layer, block, whose = at(j)
        return layer, pos[whose], block

    def down_at(j, pos):
        layer, block, whose = at(j)
        return layer, block, pos[whose], 0, 0

    across = pl.BlockSpec((None, QUARTER, tiles * T), across_at)
    down = pl.BlockSpec((None, tiles, None, T // 4, D), down_at)
    three = [across, across, down]
    q_at = [lambda j, pos: (0, 0, jnp.minimum(j, steps[0] - 1)), lambda j, pos: (0, 0, jnp.maximum(j - steps[0], 0))]
    return pl.pallas_call(
        functools.partial(adamw_kernel, tiles, steps),
        grid_spec=pltpu.PrefetchScalarGridSpec(
            num_scalar_prefetch=1,
            grid=(sum(steps),),
            in_specs=[pl.BlockSpec(memory_space=pltpu.SMEM)]
            + [pl.BlockSpec((3, QUARTER, tiles * T), q_at[i]) for i in range(len(parts))]
            + three * 3
            + [pl.BlockSpec(memory_space=pl.ANY)] * len(so_far),
            out_specs=three * 3,
        ),
        out_shape=tuple(jax.ShapeDtypeStruct(w.shape, d) for d in (BF16, F32, F32) for w in weights),
        input_output_aliases={11 + len(parts) + i: i for i in range(len(so_far))},
        compiler_params=pltpu.CompilerParams(vmem_limit_bytes=64_000_000),
        cost_estimate=pl.CostEstimate(flops=0, bytes_accessed=17 * D * T * tiles * sum(steps), transcendentals=0),
        name="adamw",
    )(pos, factor, *[part[3] for part in parts], *weights, *m, *v, *so_far)


def solution(mesh):
    swap_cores = [(0, 1), (1, 0), (2, 3), (3, 2)]
    swap_chips = [(0, 2), (2, 0), (1, 3), (3, 1)]

    def whole(x, dy, *arrays):
        weights, m, v = (arrays[i : i + 3] for i in (0, 3, 6))
        own, sibling, early, pieces, factor = gradients(x[0], dy[0], *weights)
        me = lax.axis_index("dp")
        core, chip = me % 2, me // 2
        pos = jnp.stack([core * 2 + chip, (1 - core) * 2 + chip, core * 2 + 1 - chip, (1 - core) * 2 + 1 - chip]).astype(jnp.int32)
        weights, m, v = ([*three[:2], three[2].reshape(LAYERS, NT, 4, T // 4, D)] for three in (weights, m, v))
        others = [early]
        for n in range(1, N):
            others.append(lax.ppermute(pieces[n - 1], "dp", swap_chips))
        inner = lax.ppermute(early, "dp", swap_cores)
        new = adamw(5, [(0, TILES, 0, own), (0, TILES, 1, sibling)], pos, factor, weights, m, v, ())
        first, last = PIECES[0]
        new = adamw(2, [(first, last, 2, early), (first, last, 3, inner)], pos, factor, weights, m, v, new)
        for n, (first, last) in enumerate(PIECES[1:], 1):
            other, new = lax.optimization_barrier((others[n], new))
            inner = lax.ppermute(other, "dp", swap_cores)
            new = adamw(2, [(first, last, 2, other)], pos, factor, weights, m, v, new)
            new = adamw(2, [(first, last, 3, inner)], pos, factor, weights, m, v, new)
        return tuple(one.reshape(LAYERS, FF, D) if one.ndim == 5 else one for one in new)

    return jax.shard_map(
        whole,
        mesh=mesh,
        in_specs=(P(("rep", "dp"), None, None),) * 2 + (P(None, None, None),) * 9,
        out_specs=(P("rep", None, None),) * 9,
        check_vma=False,
    )
```

```python
import functools

import jax
import jax.numpy as jnp
from jax import lax
from jax.experimental import pallas as pl
from jax.experimental.pallas import tpu as pltpu
from jax.sharding import PartitionSpec as P


MESH = pl.DeviceIdType.MESH
F32, BF16 = jnp.float32, jnp.bfloat16
TOKENS, D, FF, LAYERS = 2048, 896, 2560, 2
T = 256
NT = FF // T
TILES = LAYERS * NT
ROWS = 512
HALF, QUARTER = D // 2, D // 4
LAG = 4
PIECES = ((0, 2), (2, 8), (8, 14), (14, 17), (17, 19), (19, 20))
N = len(PIECES)
EARLY = PIECES[0][1]
COUNT = 3 * LAYERS * D * FF
FOLD = [((slice(0, 64), slice(256 * i, 256 * i + 256)), (slice(64 * i, 64 * i + 64), slice(0, 256))) for i in range(3)] + [
    ((slice(32 * i, 32 * i + 32), slice(768, 896)), (slice(192, 224), slice(128 * i, 128 * i + 128))) for i in range(2)
]


def dot(a, b, ca, cb):
    return lax.dot_general(a, b, (((ca,), (cb,)), ((), ())), preferred_element_type=F32)


def normed(h):
    wide = h.astype(F32)
    return (wide * lax.rsqrt(jnp.mean(wide * wide, -1, keepdims=True) + 1e-6)).astype(BF16)


def lanes(sq):
    by_row = jnp.sum(sq.reshape(sq.shape[0] // 8, 8, sq.shape[1]), axis=0)
    return sum(by_row[:, i * 128 : (i + 1) * 128] for i in range(sq.shape[1] // 128))


def grads_kernel(
    x_hbm, dy_hbm, wg, wu, wd,
    *refs,
):
    own, sibling, other = refs[:3]
    pieces = refs[2 : 2 + N]
    (
    factor,
    x, h, dy, a, acc, hs, dgs, dus,
    mine_gu, mine_d, r1_gu, r1_d, xs, xk, r2, squares, ss_all,
    in_sem, d_send, d_recv, x_send, x_recv, out_sem, g_send, g_recv, e_send, e_recv, s_send, s_recv,
    ) = refs[2 + N :]
    s = pl.program_id(0)
    me, rep = lax.axis_index("dp"), lax.axis_index("rep")
    core, chip = lax.rem(me, 2), lax.div(me, 2)
    partner, across = me + 1 - 2 * core, lax.rem(me + 2, 4)
    t = s - NT

    def rows_loop(body, first=0, last=TOKENS):
        for i in range(first, last, ROWS):
            body(pl.ds(i, ROWS))

    def to_partner(t):
        slot = lax.rem(t, 2)
        theirs = pl.ds(pl.multiple_of((1 - core) * HALF, 64), HALF)
        theirs_d = pl.ds(pl.multiple_of((1 - core) * (T // 2), 64), T // 2)
        make = functools.partial(pltpu.make_async_remote_copy, device_id=(rep, partner), device_id_type=MESH)
        return (
            make(mine_gu.at[slot, :, theirs, :], r1_gu.at[slot], d_send.at[slot, 0], d_recv.at[slot, 0]),
            make(mine_d.at[slot, theirs_d, :], r1_d.at[slot], d_send.at[slot, 1], d_recv.at[slot, 1]),
        )

    def to_across(t):
        slot = lax.rem(t, LAG + 1)
        make = functools.partial(pltpu.make_async_remote_copy, device_id=(rep, across), device_id_type=MESH)
        return (make(xs.at[slot], r2.at[t + LAG], x_send.at[slot], x_recv.at[t]),)

    def outs(t, piece):
        first, src = PIECES[piece][0], r2.at[t + LAG]
        everywhere = pl.ds(pl.multiple_of(t * T, T), T)
        here = pl.ds(pl.multiple_of((t - first) * T, T), T)
        make = functools.partial(pltpu.make_async_remote_copy, device_id_type=MESH)
        copies = [
            pltpu.make_async_copy(src, own.at[:, :, everywhere], out_sem.at[t, 0]),
            make(src, sibling.at[:, :, everywhere], g_send.at[t], g_recv.at[t], device_id=(rep, partner)),
        ]
        if piece:
            copies.append(pltpu.make_async_copy(src, pieces[piece].at[:, :, here], out_sem.at[t, 1]))
        else:
            copies.append(make(src, other.at[:, :, here], e_send.at[t], e_recv.at[t], device_id=(rep, across)))
        return copies

    def chip_sum(t):
        slot, xslot = lax.rem(t + 2, 2), lax.rem(t + LAG + 1, LAG + 1)
        for keep in (True, False):
            q = chip if keep else 1 - chip
            mine = pl.ds(pl.multiple_of(core * HALF + q * QUARTER, 32), QUARTER)
            got = pl.ds(pl.multiple_of(q * QUARTER, 32), QUARTER)
            mine_rows = pl.ds(pl.multiple_of(core * (T // 2) + q * (T // 4), 64), T // 4)
            got_rows = pl.ds(pl.multiple_of(q * (T // 4), 64), T // 4)
            to = xk if keep else xs
            for i in range(2):
                total = mine_gu[slot, i, mine, :].astype(F32) + r1_gu[slot, i, got, :].astype(F32)
                to[xslot, i] = total.astype(to.dtype)
            total = (mine_d[slot, mine_rows, :].astype(F32) + r1_d[slot, got_rows, :].astype(F32)).astype(to.dtype)
            for (rows, cols), (at_rows, at_cols) in FOLD:
                to[xslot, 2, at_rows, at_cols] = total[rows, cols]

    def finish(t):
        xslot = lax.rem(t + LAG + 1, LAG + 1)
        part = squares[...]
        for i in range(3):
            g = (xk[xslot, i] + r2[t + LAG, i].astype(F32)).astype(BF16)
            r2[t + LAG, i] = g
            g = g.astype(F32)
            part += lanes(g * g)
        squares[...] = jnp.where(t >= 0, part, squares[...])

    def put_out(t):
        for piece, (first, last) in enumerate(PIECES):

            @pl.when((t >= first) & (t < last))
            def _():
                for c in outs(t, piece):
                    c.start()

    @pl.when(s == 0)
    def _():
        barrier = pltpu.get_barrier_semaphore()
        for k in range(1, 4):
            pl.semaphore_signal(barrier, inc=1, device_id=(rep, lax.rem(me + k, 4)), device_id_type=MESH)
        load_x = pltpu.make_async_copy(x_hbm, x, in_sem.at[0])
        load_dy = pltpu.make_async_copy(dy_hbm, dy, in_sem.at[1])
        load_x.start()
        load_dy.start()
        load_x.wait()
        squares[...] = jnp.zeros_like(squares)

        def start(r):
            a[r, :] = normed(x[r, :])
            acc[r, :] = jnp.zeros((ROWS, D), F32)

        rows_loop(start)
        load_dy.wait()
        pl.semaphore_wait(barrier, 3)

    @pl.when(s < NT)
    def _():
        def forward(r):
            gate = dot(a[r, :], wg[...], 1, 0)
            up = dot(a[r, :], wu[...], 1, 0)
            hidden = (gate * jax.nn.sigmoid(gate) * up).astype(BF16)
            acc[r, :] += dot(hidden, wd[...], 1, 0)

        rows_loop(forward)

    @pl.when(s == NT)
    def _():
        def between(r):
            h[r, :] = x[r, :] + acc[r, :].astype(BF16)
            a[r, :] = normed(h[r, :])
            acc[r, :] = jnp.zeros((ROWS, D), F32)

        rows_loop(between)

    @pl.when(s == 2 * NT)
    def _():
        def between(r):
            da = acc[r, :].astype(BF16).astype(F32)
            wide = h[r, :].astype(F32)
            scale = lax.rsqrt(jnp.mean(wide * wide, -1, keepdims=True) + 1e-6)
            along = jnp.mean(da * wide, -1, keepdims=True)
            by_norm = da * scale - wide * (scale * scale * scale * along)
            dy[r, :] = dy[r, :] + by_norm.astype(BF16)
            a[r, :] = normed(x[r, :])

        rows_loop(between)

    @pl.when(s >= NT)
    def _():
        def hidden_grads(r):
            gate = dot(a[r, :], wg[...], 1, 0)
            up = dot(a[r, :], wu[...], 1, 0)
            dhid = dot(dy[r, :], wd[...], 1, 1).astype(BF16).astype(F32)
            sig = jax.nn.sigmoid(gate)
            silu = gate * sig
            hs[r, :] = (silu * up).astype(BF16)
            dus[r, :] = (dhid * silu).astype(BF16)
            dgs[r, :] = (dhid * up * (sig + silu * (1 - sig))).astype(BF16)

        half = TOKENS // 2
        rows_loop(hidden_grads, 0, half)

        @pl.when(t >= 1)
        def _():
            for c in to_partner(t - 1):
                c.wait()

        rows_loop(hidden_grads, half, TOKENS)
        chip_sum(t - 1)

        @pl.when(t >= 1)
        def _():
            for c in to_across(t - 1):
                c.start()

        @pl.when(t >= LAG)
        def _():
            for c in to_across(t - LAG):
                c.wait()

        @pl.when(s < 2 * NT)
        def _():
            def input_grads(r):
                by_both = jnp.concatenate([dgs[r, :], dus[r, :]], 1)
                acc[r, :] += dot(by_both, jnp.concatenate([wg[...], wu[...]], 1), 1, 1)

            rows_loop(input_grads)

        slot = lax.rem(t, 2)
        finish(t - LAG)
        mine_d[slot] = dot(hs[...], dy[...], 0, 0).astype(BF16)
        mine_gu[slot, 0] = dot(a[...], dgs[...], 0, 0).astype(BF16)
        mine_gu[slot, 1] = dot(a[...], dus[...], 0, 0).astype(BF16)
        for c in to_partner(t):
            c.start()

        @pl.when(t >= LAG)
        def _():
            put_out(t - LAG)

    @pl.when(s == NT + TILES - 1)
    def _():
        for c in to_partner(TILES - 1):
            c.wait()
        chip_sum(TILES - 1)
        for c in to_across(TILES - 1):
            c.start()

        def rest(i, carry):
            for c in to_across(i):
                c.wait()
            finish(i)
            put_out(i)
            return carry

        lax.fori_loop(TILES - LAG, TILES, rest, 0)
        ss_all[me] = squares[...]
        copies = [
            pltpu.make_async_remote_copy(
                squares, ss_all.at[me], s_send.at[k - 1], s_recv.at[me],
                device_id=(rep, lax.rem(me + k, 4)), device_id_type=MESH,
            )
            for k in range(1, 4)
        ]
        for c in copies:
            c.start()
        for c in copies:
            c.wait_send()
        for k in range(1, 4):
            who = lax.rem(me + k, 4)
            pltpu.make_async_remote_copy(
                squares, ss_all.at[who], s_send.at[k - 1], s_recv.at[who], device_id=(rep, who), device_id_type=MESH
            ).wait_recv()
        total = jnp.sum((ss_all[0] + ss_all[1]) + (ss_all[2] + ss_all[3]))
        factor[...] = jnp.minimum(1.0, 0.5 * lax.rsqrt(jnp.full((8, 128), total / COUNT + 1e-30, F32)))
        for piece, (first, last) in enumerate(PIECES):
            lax.fori_loop(first, last, lambda i, c: ([o.wait() for o in outs(i, piece)], c)[1], 0)


def gradients(x, dy, w_gate, w_up, w_down):
    any_space = pl.BlockSpec(memory_space=pl.ANY)
    layer = lambda s: lax.rem(lax.div(s, NT), 2)
    across = pl.BlockSpec((None, D, T), lambda s: (layer(s), 0, lax.rem(s, NT)))
    down = pl.BlockSpec((None, T, D), lambda s: (layer(s), lax.rem(s, NT), 0))
    sizes = [TILES, TILES] + [last - first for first, last in PIECES]
    shapes = [jax.ShapeDtypeStruct((3, QUARTER, size * T), BF16) for size in sizes]
    V, DMA = pltpu.VMEM, pltpu.SemaphoreType.DMA
    *results, factor = pl.pallas_call(
        grads_kernel,
        grid=(NT + TILES,),
        out_shape=(*shapes, jax.ShapeDtypeStruct((8, 128), F32)),
        in_specs=[any_space, any_space, across, across, down],
        out_specs=[any_space] * len(shapes) + [pl.BlockSpec((8, 128), lambda s: (0, 0))],
        scratch_shapes=[
            V((TOKENS, D), BF16), V((TOKENS, D), BF16), V((TOKENS, D), BF16), V((TOKENS, D), BF16), V((TOKENS, D), F32),
            V((TOKENS, T), BF16), V((TOKENS, T), BF16), V((TOKENS, T), BF16),
            V((2, 2, D, T), BF16), V((2, T, D), BF16),
            V((2, 2, HALF, T), BF16), V((2, T // 2, D), BF16),
            V((LAG + 1, 3, QUARTER, T), BF16), V((LAG + 1, 3, QUARTER, T), F32), V((TILES + LAG, 3, QUARTER, T), BF16),
            V((8, 128), F32), V((4, 8, 128), F32),
            DMA((2,)), DMA((2, 2)), DMA((2, 2)), DMA((LAG + 1,)), DMA((TILES,)), DMA((TILES, 2)),
            DMA((TILES,)), DMA((TILES,)), DMA((EARLY,)), DMA((EARLY,)), DMA((3,)), DMA((4,)),
        ],
        compiler_params=pltpu.CompilerParams(
            collective_id=0, has_side_effects=True, vmem_limit_bytes=67_000_000, dimension_semantics=("arbitrary",)
        ),
        cost_estimate=pl.CostEstimate(flops=17 * 2 * TOKENS * D * FF, bytes_accessed=100_000_000, transcendentals=0),
        name="grads",
    )(x, dy, w_gate, w_up, w_down)
    own, sibling, early, *pieces = results
    return own, sibling, early, pieces, factor


def adamw_kernel(tiles, steps, pos, factor, *refs):
    *qs, refs = (*refs[: len(steps)], refs[len(steps) :])
    scale, j = factor[0, 0], pl.program_id(0)

    def update(which, at_q, *at):
        (w, m, v), (new_w, new_m, new_v) = refs[which:9:3], refs[-9:][which::3]
        g = qs[0][at_q] if len(qs) == 1 else jnp.where(j < steps[0], qs[0][at_q], qs[1][at_q])
        g = g.astype(F32) * scale
        m1 = 0.9 * m[at] + 0.1 * g
        v1 = 0.95 * v[at] + 0.05 * g * g
        w0 = w[at].astype(F32)
        new_m[at] = m1
        new_v[at] = v1
        new_w[at] = (w0 - 0.02 * (m1 * lax.rsqrt(v1 + 1e-8) + 0.1 * w0)).astype(BF16)

    for which in range(2):
        update(which, which, slice(None), slice(None))
    for i in range(tiles):
        for there, (rows, cols) in FOLD:
            update(2, (2, rows, slice(cols.start + i * T, cols.stop + i * T)), i, *there)


def adamw(tiles, parts, pos, factor, weights, m, v, so_far):
    steps = [(last - first) // tiles for first, last, _, _ in parts]

    def at(j):
        (first, _, whose, _), (first1, _, whose1, _) = parts[0], parts[-1]
        later = j >= steps[0]
        first = jnp.where(later, first1 - tiles * steps[0], first) + tiles * j
        return 1 - first // NT, first % NT // tiles, jnp.where(later, whose1, whose)

    def across_at(j, pos):
        layer, block, whose = at(j)
        return layer, pos[whose], block

    def down_at(j, pos):
        layer, block, whose = at(j)
        return layer, block, pos[whose], 0, 0

    across = pl.BlockSpec((None, QUARTER, tiles * T), across_at)
    down = pl.BlockSpec((None, tiles, None, T // 4, D), down_at)
    three = [across, across, down]
    q_at = [lambda j, pos: (0, 0, jnp.minimum(j, steps[0] - 1)), lambda j, pos: (0, 0, jnp.maximum(j - steps[0], 0))]
    return pl.pallas_call(
        functools.partial(adamw_kernel, tiles, steps),
        grid_spec=pltpu.PrefetchScalarGridSpec(
            num_scalar_prefetch=1,
            grid=(sum(steps),),
            in_specs=[pl.BlockSpec(memory_space=pltpu.SMEM)]
            + [pl.BlockSpec((3, QUARTER, tiles * T), q_at[i]) for i in range(len(parts))]
            + three * 3
            + [pl.BlockSpec(memory_space=pl.ANY)] * len(so_far),
            out_specs=three * 3,
        ),
        out_shape=tuple(jax.ShapeDtypeStruct(w.shape, d) for d in (BF16, F32, F32) for w in weights),
        input_output_aliases={11 + len(parts) + i: i for i in range(len(so_far))},
        compiler_params=pltpu.CompilerParams(vmem_limit_bytes=64_000_000),
        cost_estimate=pl.CostEstimate(flops=0, bytes_accessed=17 * D * T * tiles * sum(steps), transcendentals=0),
        name="adamw",
    )(pos, factor, *[part[3] for part in parts], *weights, *m, *v, *so_far)


def solution(mesh):
    swap_cores = [(0, 1), (1, 0), (2, 3), (3, 2)]
    swap_chips = [(0, 2), (2, 0), (1, 3), (3, 1)]

    def whole(x, dy, *arrays):
        weights, m, v = (arrays[i : i + 3] for i in (0, 3, 6))
        own, sibling, early, pieces, factor = gradients(x[0], dy[0], *weights)
        me = lax.axis_index("dp")
        core, chip = me % 2, me // 2
        pos = jnp.stack([core * 2 + chip, (1 - core) * 2 + chip, core * 2 + 1 - chip, (1 - core) * 2 + 1 - chip]).astype(jnp.int32)
        weights, m, v = ([*three[:2], three[2].reshape(LAYERS, NT, 4, T // 4, D)] for three in (weights, m, v))
        others = [early]
        for n in range(1, N):
            others.append(lax.ppermute(pieces[n - 1], "dp", swap_chips))
        inner = lax.ppermute(early, "dp", swap_cores)
        new = adamw(5, [(0, TILES, 0, own), (0, TILES, 1, sibling)], pos, factor, weights, m, v, ())
        first, last = PIECES[0]
        new = adamw(1, [(first, last, 2, early), (first, last, 3, inner)], pos, factor, weights, m, v, new)
        for n, (first, last) in enumerate(PIECES[1:], 1):
            other, new = lax.optimization_barrier((others[n], new))
            inner = lax.ppermute(other, "dp", swap_cores)
            tiles = 1 if last - first < 4 else 2
            new = adamw(tiles, [(first, last, 2, other)], pos, factor, weights, m, v, new)
            new = adamw(tiles, [(first, last, 3, inner)], pos, factor, weights, m, v, new)
        return tuple(one.reshape(LAYERS, FF, D) if one.ndim == 5 else one for one in new)

    return jax.shard_map(
        whole,
        mesh=mesh,
        in_specs=(P(("rep", "dp"), None, None),) * 2 + (P(None, None, None),) * 9,
        out_specs=(P("rep", None, None),) * 9,
        check_vma=False,
    )
```
